32 devices in a mesh: parts: 2 (over y), leaf: 4 (over z), mid: 2 (over x), top: 2 (over core).
Axes of the slice: x: 2, y: 2, z: 4, core: 2. Of those that a mesh axis runs over, the one named last changes fastest.
Arguments:
- leaf_precision: float32 [8, 2, 2, 128, 128], P(('parts', 'leaf'), 'mid', 'top'), parts along dimension 0, may hold values from -40 to 40, as said below
- basis_fine: float32 [8, 2, 2, 128, 128], P(('parts', 'leaf'), 'mid', 'top'), parts along dimension 0, may hold values from -1 to 1
- basis_mid: float32 [8, 2, 2, 128, 128], P(('parts', 'leaf'), 'mid', 'top'), parts along dimension 0, may hold values from -1 to 1
- basis_coarse: float32 [8, 2, 2, 128, 128], P(('parts', 'leaf'), 'mid', 'top'), parts along dimension 0, may hold values from -1 to 1
- core_fine: float32 [128, 128], replicated, may hold values from -20 to 20, as said below
- core_mid: float32 [128, 128], replicated, may hold values from -20 to 20, as said below
- core_coarse: float32 [128, 128], replicated, may hold values from -20 to 20, as said below
- observations: float32 [8, 2, 2, 128, 128], P(('parts', 'leaf'), 'mid', 'top'), parts along dimension 0, may hold values from -20 to 20
Outputs:
- solution: float32 [8, 2, 2, 128, 128], P(('parts', 'leaf'), 'mid', 'top'), parts along dimension 0
The draws below stay inside these ranges and needn't reach their ends.
There are 2 independent parts, one for each index of `parts`. The reference program is written for one: setup_inputs(seed, part) draws one part's arguments, and reference() takes and returns one part's arrays. A program takes and returns all parts, laid end to end along the dimension named above; an argument that names none is the same for every part. Nothing has to cross between parts.
Inputs may be any that keep to these rules, and one draw needn't show every extreme that they name: Every leaf_precision[l, m, t] is symmetric positive definite. `core_fine`: symmetric positive definite. `core_mid`: symmetric positive definite. `core_coarse`: symmetric positive definite.
All inputs are finite; a program needn't handle non-finite values.
Results may differ from the reference program's by a relative error of at most 0.00005.
Values sent between devices are 32-bit elements; how exact they have to be, the bound alone decides.
A program may use at most 64 MiB of HBM per device.

```python
import jax
import jax.numpy as jnp
from jax import lax

ROWS = 128
R = 128
COLS = 128
GROUP_FINE = 512
GROUP_MID = 1024
POINTS = 2048
N_LEAF = 4
N_MID = 2
N_TOP = 2


def log_between(key, shape, lower, upper):
    return jnp.exp(jax.random.uniform(key, shape, jnp.float32, jnp.log(lower), jnp.log(upper)))


def draw_leaf_precision(key, part):
    key_mix, key_diag = jax.random.split(jax.random.fold_in(key, 1), 2)
    shape = (N_LEAF, N_MID, N_TOP, ROWS, ROWS)
    mixing = jax.random.normal(key_mix, shape, jnp.float32) / jnp.sqrt(jnp.float32(ROWS))
    product = jnp.einsum('lmtij,lmtkj->lmtik', mixing, mixing, precision=lax.Precision.HIGHEST)
    diagonal = log_between(key_diag, shape[:-1], 0.5, 2.0)
    eye_rows = jnp.eye(ROWS, dtype=jnp.float32)
    result = 0.5 * product + diagonal[..., :, None] * eye_rows
    return result


def core_matrix(key, salt):
    key_mix, key_diag = jax.random.split(jax.random.fold_in(key, salt), 2)
    mixing = jax.random.normal(key_mix, (R, R), jnp.float32)
    product = jnp.dot(mixing, mixing.T, precision=lax.Precision.HIGHEST) / R
    diagonal = log_between(key_diag, (R,), 0.5, 2.0)
    result = 0.3 * product + jnp.diag(diagonal)
    return result


def draw_core_fine(key, part):
    return core_matrix(key, 11)


def draw_core_mid(key, part):
    return core_matrix(key, 12)


def draw_core_coarse(key, part):
    return core_matrix(key, 13)


def basis_level(key, salt, group_rows):
    key_entry = jax.random.fold_in(jax.random.fold_in(key, salt), 0)
    shape = (N_LEAF, N_MID, N_TOP, ROWS, R)
    entries = jnp.clip(jax.random.normal(key_entry, shape, jnp.float32), -5.0, 5.0)
    return entries / jnp.sqrt(jnp.float32(group_rows))


def draw_basis_fine(key, part):
    return basis_level(key, 101, GROUP_FINE)


def draw_basis_mid(key, part):
    return basis_level(key, 102, GROUP_MID)


def draw_basis_coarse(key, part):
    return basis_level(key, 103, POINTS)


def draw_observations(key, part):
    precise = lax.Precision.HIGHEST
    fine_basis = basis_level(key, 101, GROUP_FINE)
    mid_basis = basis_level(key, 102, GROUP_MID)
    coarse_basis = basis_level(key, 103, POINTS)
    key_fine, key_mid, key_coarse, key_noise = jax.random.split(jax.random.fold_in(key, 200), 4)
    fine_weight = jnp.clip(jax.random.normal(key_fine, (N_MID, N_TOP, R, COLS), jnp.float32), -5.0, 5.0) * (0.7 * jnp.sqrt(jnp.float32(GROUP_FINE) / R))
    mid_weight = jnp.clip(jax.random.normal(key_mid, (N_TOP, R, COLS), jnp.float32), -5.0, 5.0) * (0.7 * jnp.sqrt(jnp.float32(GROUP_MID) / R))
    coarse_weight = jnp.clip(jax.random.normal(key_coarse, (R, COLS), jnp.float32), -5.0, 5.0) * (0.7 * jnp.sqrt(jnp.float32(POINTS) / R))
    noise = jnp.clip(jax.random.normal(key_noise, (N_LEAF, N_MID, N_TOP, ROWS, COLS), jnp.float32), -5.0, 5.0)
    signal = jnp.einsum('lmtrk,mtkc->lmtrc', fine_basis, fine_weight, precision=precise)
    signal = signal + jnp.einsum('lmtrk,tkc->lmtrc', mid_basis, mid_weight, precision=precise)
    signal = signal + jnp.einsum('lmtrk,kc->lmtrc', coarse_basis, coarse_weight, precision=precise)
    return jnp.clip(signal + noise, -20.0, 20.0)


def setup_inputs(seed: int = 0, part: int = 0) -> dict:
    splits = jax.random.split(jax.random.key(seed), 9)
    part_keys = jax.random.split(jax.random.fold_in(splits[8], part), 9)
    return {
        "leaf_precision": draw_leaf_precision(jax.random.fold_in(jax.random.fold_in(splits[8], part), 71), part),
        "basis_fine": draw_basis_fine(jax.random.fold_in(jax.random.fold_in(splits[8], part), 71), part),
        "basis_mid": draw_basis_mid(jax.random.fold_in(jax.random.fold_in(splits[8], part), 71), part),
        "basis_coarse": draw_basis_coarse(jax.random.fold_in(jax.random.fold_in(splits[8], part), 71), part),
        "core_fine": draw_core_fine(jax.random.fold_in(splits[8], 71), part),
        "core_mid": draw_core_mid(jax.random.fold_in(splits[8], 71), part),
        "core_coarse": draw_core_coarse(jax.random.fold_in(splits[8], 71), part),
        "observations": draw_observations(jax.random.fold_in(jax.random.fold_in(splits[8], part), 71), part),
    }


def solve_core(matrix, right_side):
    return jax.scipy.linalg.cho_solve((jnp.linalg.cholesky(matrix), True), right_side)

def batched_solve(matrix, right_side):
    lead = matrix.shape[:-2]
    flat_matrix = matrix.reshape((-1,) + matrix.shape[-2:])
    flat_right = right_side.reshape((-1,) + right_side.shape[-2:])
    result = jax.vmap(solve_core)(flat_matrix, flat_right)
    return result.reshape(lead + right_side.shape[-2:])

def reference(leaf_precision, basis_fine, basis_mid, basis_coarse, core_fine, core_mid, core_coarse, observations):
    precise = lax.Precision.HIGHEST
    core_rank = basis_fine.shape[4]
    stacked = jnp.concatenate([basis_fine, basis_mid, basis_coarse, observations], axis=4)
    solved = jnp.einsum('lmtij,lmtjc->lmtic', leaf_precision, stacked, precision=precise)
    fine_gram = jnp.einsum('lmtrk,lmtrc->mtkc', basis_fine, solved, precision=precise)
    fine_coef = batched_solve(core_fine[None, None] + fine_gram[..., :core_rank], fine_gram[..., core_rank:])
    after_fine = solved[..., core_rank:] - jnp.einsum('lmtrk,mtkc->lmtrc', solved[..., :core_rank], fine_coef, precision=precise)
    mid_gram = jnp.einsum('lmtrk,lmtrc->tkc', basis_mid, after_fine, precision=precise)
    mid_coef = batched_solve(core_mid[None] + mid_gram[..., :core_rank], mid_gram[..., core_rank:])
    after_mid = after_fine[..., core_rank:] - jnp.einsum('lmtrk,tkc->lmtrc', after_fine[..., :core_rank], mid_coef, precision=precise)
    coarse_gram = jnp.einsum('lmtrk,lmtrc->kc', basis_coarse, after_mid, precision=precise)
    coarse_coef = solve_core(core_coarse + coarse_gram[:, :core_rank], coarse_gram[:, core_rank:])
    return after_mid[..., core_rank:] - jnp.einsum('lmtrk,kc->lmtrc', after_mid[..., :core_rank], coarse_coef, precision=precise)
```

```python
import functools

import jax
import jax.numpy as jnp
from jax import lax
from jax.experimental import pallas as pl
from jax.experimental.pallas import tpu as pltpu
from jax.sharding import PartitionSpec as P

MESH = pl.DeviceIdType.MESH
PANEL = 8


def dot(left_hand, right_side):
    return jnp.dot(
        left_hand, right_side, precision=lax.Precision.HIGHEST, preferred_element_type=jnp.float32
    )


def split3(x):
    high = x.astype(jnp.bfloat16).astype(jnp.float32)
    rest = x - high
    mid = rest.astype(jnp.bfloat16).astype(jnp.float32)
    low = (rest - mid).astype(jnp.bfloat16).astype(jnp.float32)
    return high, mid, low


def rank_update(panel, scaled):
    p1, p2, p3 = split3(panel)
    r1, r2, r3 = split3(scaled)
    left_hand = jnp.concatenate([p1, p1, p2, p2, p1, p3], axis=0).T.astype(jnp.bfloat16)
    right_side = jnp.concatenate([r1, r2, r1, r2, r3, r1], axis=0).astype(jnp.bfloat16)
    return jnp.dot(left_hand, right_side, preferred_element_type=jnp.float32)


def negated_inverse(a_ref, matrix):
    size = matrix.shape[0]
    zero = jnp.zeros((PANEL, size), jnp.float32)
    a_ref[pl.ds(0, PANEL), :] = zero
    a_ref[pl.ds(PANEL, size), :] = matrix
    a_ref[pl.ds(PANEL + size, PANEL), :] = zero
    lane = lax.broadcasted_iota(jnp.int32, (PANEL, size), 1)
    sub = lax.broadcasted_iota(jnp.int32, (PANEL, size), 0)
    lane_full = lax.broadcasted_iota(jnp.int32, (size, size), 1)

    def columns(block, k):
        return [
            jnp.broadcast_to(
                jnp.sum(jnp.where(lane == k * PANEL + j, block, 0.0), axis=1, keepdims=True),
                block.shape,
            )
            for j in range(PANEL)
        ]

    def apply(k, panel, scaled):
        inside = (lane_full >= k * PANEL) & (lane_full < (k + 1) * PANEL)
        current = a_ref[pl.ds(PANEL, size), :]
        a_ref[pl.ds(PANEL, size), :] = jnp.where(inside, 0.0, current) - rank_update(panel, scaled)
        a_ref[pl.ds(pl.multiple_of((k + 1) * PANEL, PANEL), PANEL), :] = scaled

    def body(k, carry):
        panel_before, scaled_before, panel = carry
        apply(k - 1, panel_before, scaled_before)
        inside = (lane >= k * PANEL) & (lane < (k + 1) * PANEL)
        cols = columns(panel, k)
        x = jnp.where(inside, jnp.where(lane - k * PANEL == sub, 1.0, 0.0), panel)
        for i in range(PANEL):
            pivot = 1.0 / jnp.broadcast_to(cols[i][i : i + 1], x.shape)
            here = sub == i

            def step(v):
                row = jnp.broadcast_to(v[i : i + 1], v.shape) * pivot
                return jnp.where(here, row, v - cols[i] * row)

            x_new = step(x)
            for j in range(i + 1, PANEL):
                cols[j] = step(cols[j])
            x = x_new
        scaled = jnp.where(inside, -x, x)
        following = a_ref[pl.ds(pl.multiple_of((k + 2) * PANEL, PANEL), PANEL), :]
        coefs = columns(following, k)
        panel_next = jnp.where(inside, 0.0, following)
        for j in range(PANEL):
            panel_next = panel_next - coefs[j] * jnp.broadcast_to(scaled[j : j + 1], x.shape)
        return panel, scaled, panel_next

    steps = size // PANEL
    panel, scaled, _ = lax.fori_loop(0, steps, body, (zero, zero, matrix[:PANEL]))
    apply(steps - 1, panel, scaled)
    return a_ref[pl.ds(PANEL, size), :]


def kernel(
    n_leaf, n_mid, n_top,
    prec_ref, fine_ref, mid_ref, coarse_ref, core_fine_ref, core_mid_ref, core_coarse_ref, obs_ref,
    out_ref,
    a_ref, ff_ref, ff_in, bulk_ref, rs_in, ag_ref, piece_ref, piece_in, quarter_ref, s_ref,
    top_ref, top_in,
    ff_send, ff_recv, rs_send, rs_recv, ag_send, ag_recv, mid_send, mid_recv,
    s_send, s_recv, top_send, top_recv,
):
    r = fine_ref.shape[1]
    rows = r // n_leaf
    leaf, mid, top = lax.axis_index("leaf"), lax.axis_index("mid"), lax.axis_index("top")
    barrier = pltpu.get_barrier_semaphore()

    def peer(axis, index, count, step):
        return {axis: lax.rem(index + step, count)}

    for axis, index, count in (("leaf", leaf, n_leaf), ("mid", mid, n_mid), ("top", top, n_top)):
        for step in range(1, count):
            pl.semaphore_signal(
                barrier, inc=1, device_id=peer(axis, index, count, step), device_id_type=MESH
            )

    def send(src, dst, send_sem, recv_sem, axis, index, count, step):
        copy = pltpu.make_async_remote_copy(
            src_ref=src, dst_ref=dst, send_sem=send_sem.at[step - 1], recv_sem=recv_sem.at[step - 1],
            device_id=peer(axis, index, count, step), device_id_type=MESH,
        )
        copy.start()
        return copy

    prec = prec_ref[...]
    fine, middle, coarse = fine_ref[...], mid_ref[...], coarse_ref[...]
    solved_f = dot(prec, fine)
    fine_t = fine.T
    ff = dot(fine_t, solved_f)
    ff_ref[...] = ff
    pl.semaphore_wait(barrier, (n_leaf - 1) + (n_mid - 1) + (n_top - 1))
    ff_copies = [
        send(ff_ref, ff_in.at[step - 1], ff_send, ff_recv, "leaf", leaf, n_leaf, step)
        for step in range(1, n_leaf)
    ]
    mid_t, coarse_t = middle.T, coarse.T
    solved_m, solved_c, solved_y = dot(prec, middle), dot(prec, coarse), dot(prec, obs_ref[...])
    for place, (left_hand, right_side) in enumerate((
        (mid_t, solved_f), (coarse_t, solved_f), (fine_t, solved_y),
        (mid_t, solved_m), (mid_t, solved_c), (mid_t, solved_y),
        (coarse_t, solved_c), (coarse_t, solved_y),
    )):
        bulk_ref[:, place * r : (place + 1) * r] = dot(left_hand, right_side)
    rs_copies = []
    for step in range(1, n_leaf):
        target = lax.rem(leaf + step, n_leaf)
        rs_copies.append(send(
            bulk_ref.at[pl.ds(pl.multiple_of(target * rows, rows), rows), :], rs_in.at[step - 1],
            rs_send, rs_recv, "leaf", leaf, n_leaf, step,
        ))
    own_rows = pl.ds(pl.multiple_of(leaf * rows, rows), rows)

    total = core_fine_ref[...] + ff
    for step in range(1, n_leaf):
        ff_copies[step - 1].wait()
        total = total + ff_in[step - 1]
    fine_inverse = negated_inverse(a_ref, total)

    part = bulk_ref[own_rows, :]
    for step in range(1, n_leaf):
        rs_copies[step - 1].wait()
        part = part + rs_in[step - 1]
    quarter_ref[...] = part[:, : 3 * r]
    ag_copies = [
        send(quarter_ref, ag_ref.at[own_rows, :], ag_send, ag_recv, "leaf", leaf, n_leaf, step)
        for step in range(1, n_leaf)
    ]
    ag_ref[own_rows, :] = part[:, : 3 * r]
    for copy in ag_copies:
        copy.wait()
    w_m = dot(fine_inverse, ag_ref[:, :r].T)
    w_c = dot(fine_inverse, ag_ref[:, r : 2 * r].T)
    w_y = dot(fine_inverse, ag_ref[:, 2 * r : 3 * r])
    q_m, q_c = part[:, :r], part[:, r : 2 * r]
    for place, (left_hand, right_side) in enumerate((
        (q_m, w_m), (q_m, w_c), (q_m, w_y), (q_c, w_c), (q_c, w_y),
    )):
        piece_ref[:, place * r : (place + 1) * r] = (
            part[:, (3 + place) * r : (4 + place) * r] + dot(left_hand, right_side)
        )
    mid_copies = [
        send(piece_ref, piece_in.at[step - 1], mid_send, mid_recv, "mid", mid, n_mid, step)
        for step in range(1, n_mid)
    ]
    piece = piece_ref[...]
    for step in range(1, n_mid):
        mid_copies[step - 1].wait()
        piece = piece + piece_in[step - 1]
    piece_ref[...] = piece
    s_copies = [
        send(piece_ref, s_ref.at[own_rows, :], s_send, s_recv, "leaf", leaf, n_leaf, step)
        for step in range(1, n_leaf)
    ]
    s_ref[own_rows, :] = piece
    for copy in s_copies:
        copy.wait()

    mid_inverse = negated_inverse(a_ref, core_mid_ref[...] + s_ref[:, :r])
    cross = s_ref[:, r : 2 * r]
    v_c, v_y = dot(mid_inverse, cross), dot(mid_inverse, s_ref[:, 2 * r : 3 * r])
    cross_t = cross.T
    cc = s_ref[:, 3 * r : 4 * r] + dot(cross_t, v_c)
    cy = s_ref[:, 4 * r : 5 * r] + dot(cross_t, v_y)
    top_ref[:, :r] = cc
    top_ref[:, r:] = cy
    top_copies = [
        send(top_ref, top_in.at[step - 1], top_send, top_recv, "top", top, n_top, step)
        for step in range(1, n_top)
    ]
    for step in range(1, n_top):
        top_copies[step - 1].wait()
        cc = cc + top_in[step - 1, :, :r]
        cy = cy + top_in[step - 1, :, r:]
    coarse_inverse = negated_inverse(a_ref, core_coarse_ref[...] + cc)
    x_c = -dot(coarse_inverse, cy)
    x_m = dot(v_c, x_c) - v_y
    x_f = dot(w_m, x_m) + dot(w_c, x_c) - w_y
    out_ref[...] = solved_y - dot(solved_f, x_f) - dot(solved_m, x_m) - dot(solved_c, x_c)


def local(n_leaf, n_mid, n_top, *operands):
    blocks = [x.reshape(x.shape[-2:]) for x in operands]
    r = blocks[1].shape[1]
    rows = r // n_leaf
    f32 = jnp.float32
    dma = pltpu.SemaphoreType.DMA
    answer = pl.pallas_call(
        functools.partial(kernel, n_leaf, n_mid, n_top),
        out_shape=jax.ShapeDtypeStruct(blocks[-1].shape, f32),
        in_specs=[pl.BlockSpec(memory_space=pltpu.VMEM)] * len(blocks),
        out_specs=pl.BlockSpec(memory_space=pltpu.VMEM),
        scratch_shapes=[
            pltpu.VMEM((r + 2 * PANEL, r), f32),
            pltpu.VMEM((r, r), f32),
            pltpu.VMEM((n_leaf - 1, r, r), f32),
            pltpu.VMEM((r, 8 * r), f32),
            pltpu.VMEM((n_leaf - 1, rows, 8 * r), f32),
            pltpu.VMEM((r, 3 * r), f32),
            pltpu.VMEM((rows, 5 * r), f32),
            pltpu.VMEM((n_mid - 1, rows, 5 * r), f32),
            pltpu.VMEM((rows, 3 * r), f32),
            pltpu.VMEM((r, 5 * r), f32),
            pltpu.VMEM((r, 2 * r), f32),
            pltpu.VMEM((n_top - 1, r, 2 * r), f32),
            dma((n_leaf - 1,)), dma((n_leaf - 1,)),
            dma((n_leaf - 1,)), dma((n_leaf - 1,)),
            dma((n_leaf - 1,)), dma((n_leaf - 1,)),
            dma((n_mid - 1,)), dma((n_mid - 1,)),
            dma((n_leaf - 1,)), dma((n_leaf - 1,)),
            dma((n_top - 1,)), dma((n_top - 1,)),
        ],
        compiler_params=pltpu.CompilerParams(collective_id=0, has_side_effects=True),
    )(*blocks)
    return answer[None, None, None]


def solution(mesh):
    spread = P(("parts", "leaf"), "mid", "top", None, None)
    sizes = (mesh.shape["leaf"], mesh.shape["mid"], mesh.shape["top"])
    return jax.shard_map(
        functools.partial(local, *sizes),
        mesh=mesh,
        in_specs=(spread, spread, spread, spread, P(), P(), P(), spread),
        out_specs=spread,
        check_vma=False,
    )
```

```python
import functools

import jax
import jax.numpy as jnp
from jax import lax
from jax.experimental import pallas as pl
from jax.experimental.pallas import tpu as pltpu
from jax.sharding import PartitionSpec as P

MESH = pl.DeviceIdType.MESH
PANEL = 8


def dot(left_hand, right_side):
    return jnp.dot(
        left_hand, right_side, precision=lax.Precision.HIGHEST, preferred_element_type=jnp.float32
    )


def split3(x):
    high = x.astype(jnp.bfloat16).astype(jnp.float32)
    rest = x - high
    mid = rest.astype(jnp.bfloat16).astype(jnp.float32)
    low = (rest - mid).astype(jnp.bfloat16).astype(jnp.float32)
    return high, mid, low


def rank_update(panel, scaled):
    p1, p2, p3 = split3(panel)
    r1, r2, r3 = split3(scaled)
    left_hand = jnp.concatenate([p1, p1, p2, p2, p1, p3], axis=0).T.astype(jnp.bfloat16)
    right_side = jnp.concatenate([r1, r2, r1, r2, r3, r1], axis=0).astype(jnp.bfloat16)
    return jnp.dot(left_hand, right_side, preferred_element_type=jnp.float32)


def negated_inverse(a_ref, matrix):
    size = matrix.shape[0]
    zero = jnp.zeros((PANEL, size), jnp.float32)
    a_ref[pl.ds(0, PANEL), :] = zero
    a_ref[pl.ds(PANEL, size), :] = matrix
    a_ref[pl.ds(PANEL + size, PANEL), :] = zero
    lane = lax.broadcasted_iota(jnp.int32, (PANEL, size), 1)
    sub = lax.broadcasted_iota(jnp.int32, (PANEL, size), 0)
    lane_full = lax.broadcasted_iota(jnp.int32, (size, size), 1)

    def columns(block, k):
        return [
            jnp.broadcast_to(
                jnp.sum(jnp.where(lane == k * PANEL + j, block, 0.0), axis=1, keepdims=True),
                block.shape,
            )
            for j in range(PANEL)
        ]

    def apply(k, panel, scaled):
        inside = (lane_full >= k * PANEL) & (lane_full < (k + 1) * PANEL)
        current = a_ref[pl.ds(PANEL, size), :]
        a_ref[pl.ds(PANEL, size), :] = jnp.where(inside, 0.0, current) - rank_update(panel, scaled)
        a_ref[pl.ds(pl.multiple_of((k + 1) * PANEL, PANEL), PANEL), :] = scaled

    def body(k, carry):
        panel_before, scaled_before, panel = carry
        apply(k - 1, panel_before, scaled_before)
        inside = (lane >= k * PANEL) & (lane < (k + 1) * PANEL)
        cols = columns(panel, k)
        x = jnp.where(inside, jnp.where(lane - k * PANEL == sub, 1.0, 0.0), panel)
        for i in range(PANEL):
            pivot = 1.0 / jnp.broadcast_to(cols[i][i : i + 1], x.shape)
            here = sub == i

            def step(v):
                row = jnp.broadcast_to(v[i : i + 1], v.shape) * pivot
                return jnp.where(here, row, v - cols[i] * row)

            x_new = step(x)
            for j in range(i + 1, PANEL):
                cols[j] = step(cols[j])
            x = x_new
        scaled = jnp.where(inside, -x, x)
        following = a_ref[pl.ds(pl.multiple_of((k + 2) * PANEL, PANEL), PANEL), :]
        coefs = columns(following, k)
        panel_next = jnp.where(inside, 0.0, following)
        for j in range(PANEL):
            panel_next = panel_next - coefs[j] * jnp.broadcast_to(scaled[j : j + 1], x.shape)
        return panel, scaled, panel_next

    steps = size // PANEL
    panel, scaled, _ = lax.fori_loop(0, steps, body, (zero, zero, matrix[:PANEL]))
    apply(steps - 1, panel, scaled)
    return a_ref[pl.ds(PANEL, size), :]


def kernel(
    n_leaf, n_mid, n_top,
    prec_ref, fine_ref, mid_ref, coarse_ref, core_fine_ref, core_mid_ref, core_coarse_ref, obs_ref,
    out_ref,
    a_ref, bulk_ref, rs_in, part_ref, ag_ref, piece_ref, piece_in, quarter_ref, s_ref, top_ref, top_in,
    rs_send, rs_recv, ag_send, ag_recv, mid_send, mid_recv, s_send, s_recv, top_send, top_recv,
):
    r = fine_ref.shape[1]
    rows = r // n_leaf
    leaf, mid, top = lax.axis_index("leaf"), lax.axis_index("mid"), lax.axis_index("top")
    own_rows = pl.ds(pl.multiple_of(leaf * rows, rows), rows)
    barrier = pltpu.get_barrier_semaphore()
    places = {"leaf": (leaf, n_leaf), "mid": (mid, n_mid), "top": (top, n_top)}

    def peer(axis, step):
        index, count = places[axis]
        return {axis: lax.rem(index + step, count)}

    for axis in places:
        for step in range(1, places[axis][1]):
            pl.semaphore_signal(barrier, inc=1, device_id=peer(axis, step), device_id_type=MESH)

    def send(src, dst, sems, phase, axis, step):
        copy = pltpu.make_async_remote_copy(
            src_ref=src, dst_ref=dst,
            send_sem=sems[0].at[phase, step - 1], recv_sem=sems[1].at[phase, step - 1],
            device_id=peer(axis, step), device_id_type=MESH,
        )
        copy.start()
        return copy

    def span(blocks):
        return slice(blocks[0] * r, blocks[1] * r)

    def scatter(phase, blocks):
        copies = []
        for step in range(1, n_leaf):
            target = lax.rem(leaf + step, n_leaf)
            target_rows = pl.ds(pl.multiple_of(target * rows, rows), rows)
            copies.append(send(
                bulk_ref.at[target_rows, span(blocks)], rs_in.at[step - 1, :, span(blocks)],
                (rs_send, rs_recv), phase, "leaf", step,
            ))
        return copies, blocks

    def collect(handle):
        copies, blocks = handle
        total = bulk_ref[own_rows, span(blocks)]
        for step in range(1, n_leaf):
            copies[step - 1].wait()
            total = total + rs_in[step - 1, :, span(blocks)]
        return total

    def gather(source, target, sems, phase, blocks, value):
        source[:, span(blocks)] = value
        copies = [
            send(
                source.at[:, span(blocks)], target.at[own_rows, span(blocks)],
                sems, phase, "leaf", step,
            )
            for step in range(1, n_leaf)
        ]
        target[own_rows, span(blocks)] = value
        return copies

    def exchange(axis, source, target, sems, phase, blocks, value):
        source[:, span(blocks)] = value
        copies = [
            send(
                source.at[:, span(blocks)], target.at[step - 1, :, span(blocks)],
                sems, phase, axis, step,
            )
            for step in range(1, places[axis][1])
        ]
        return copies, target, blocks, value

    def add_up(handle):
        copies, target, blocks, total = handle
        for step, copy in enumerate(copies):
            copy.wait()
            total = total + target[step, :, span(blocks)]
        return total

    def wait_all(copies):
        for copy in copies:
            copy.wait()

    def put(place, value):
        bulk_ref[:, place * r : (place + 1) * r] = value

    prec = prec_ref[...]
    fine, middle, coarse = fine_ref[...], mid_ref[...], coarse_ref[...]
    solved_f = dot(prec, fine)
    fine_t = fine.T
    put(0, dot(fine_t, solved_f))
    pl.semaphore_wait(barrier, (n_leaf - 1) + (n_mid - 1) + (n_top - 1))
    rs_ff = scatter(0, (0, 1))
    mid_t, coarse_t = middle.T, coarse.T
    solved_y = dot(prec, obs_ref[...])
    put(1, dot(mid_t, solved_f))
    put(2, dot(coarse_t, solved_f))
    put(3, dot(fine_t, solved_y))
    rs_f = scatter(1, (1, 4))
    solved_m, solved_c = dot(prec, middle), dot(prec, coarse)
    put(4, dot(mid_t, solved_m))
    put(5, dot(mid_t, solved_c))
    put(6, dot(mid_t, solved_y))
    put(7, dot(coarse_t, solved_c))
    put(8, dot(coarse_t, solved_y))

    first = (ag_send, ag_recv)
    ag_ff = gather(part_ref, ag_ref, first, 0, (0, 1), collect(rs_ff))
    rs_m = scatter(2, (4, 7))
    part_f = collect(rs_f)
    ag_f = gather(part_ref, ag_ref, first, 1, (1, 4), part_f)
    rs_c = scatter(3, (7, 9))

    wait_all(ag_ff)
    fine_inverse = negated_inverse(a_ref, core_fine_ref[...] + ag_ref[:, :r])
    wait_all(ag_f)
    q_m, q_c = part_f[:, :r], part_f[:, r : 2 * r]
    w_m = dot(fine_inverse, ag_ref[:, r : 2 * r].T)
    part_m = collect(rs_m)
    between, second = (mid_send, mid_recv), (s_send, s_recv)
    x_mm = exchange("mid", piece_ref, piece_in, between, 0, (0, 1), part_m[:, :r] + dot(q_m, w_m))
    w_c = dot(fine_inverse, ag_ref[:, 2 * r : 3 * r].T)
    w_y = dot(fine_inverse, ag_ref[:, 3 * r : 4 * r])
    cross_piece = jnp.concatenate(
        [part_m[:, r : 2 * r] + dot(q_m, w_c), part_m[:, 2 * r :] + dot(q_m, w_y)], axis=1
    )
    x_mc = exchange("mid", piece_ref, piece_in, between, 1, (1, 3), cross_piece)
    ag_mm = gather(quarter_ref, s_ref, second, 0, (0, 1), add_up(x_mm))
    ag_mc = gather(quarter_ref, s_ref, second, 1, (1, 3), add_up(x_mc))
    part_c = collect(rs_c)
    coarse_piece = jnp.concatenate(
        [part_c[:, :r] + dot(q_c, w_c), part_c[:, r:] + dot(q_c, w_y)], axis=1
    )
    x_cc = exchange("mid", piece_ref, piece_in, between, 2, (3, 5), coarse_piece)
    coarse_sum = add_up(x_cc)
    ag_cc = gather(quarter_ref, s_ref, second, 2, (3, 4), coarse_sum[:, :r])
    ag_cy = gather(quarter_ref, s_ref, second, 3, (4, 5), coarse_sum[:, r:])

    wait_all(ag_mm)
    mid_inverse = negated_inverse(a_ref, core_mid_ref[...] + s_ref[:, :r])
    wait_all(ag_mc)
    cross = s_ref[:, r : 2 * r]
    cross_t = cross.T
    v_c = dot(mid_inverse, cross)
    last = (top_send, top_recv)
    cross_cc = dot(cross_t, v_c)
    wait_all(ag_cc)
    x_top = exchange("top", top_ref, top_in, last, 0, (0, 1), s_ref[:, 3 * r : 4 * r] + cross_cc)
    v_y = dot(mid_inverse, s_ref[:, 2 * r : 3 * r])
    cross_cy = dot(cross_t, v_y)
    wait_all(ag_cy)
    x_right = exchange("top", top_ref, top_in, last, 1, (1, 2), s_ref[:, 4 * r : 5 * r] + cross_cy)
    coarse_inverse = negated_inverse(a_ref, core_coarse_ref[...] + add_up(x_top))
    x_c = -dot(coarse_inverse, add_up(x_right))
    x_m = dot(v_c, x_c) - v_y
    x_f = dot(w_m, x_m) + dot(w_c, x_c) - w_y
    out_ref[...] = solved_y - dot(solved_f, x_f) - dot(solved_m, x_m) - dot(solved_c, x_c)


def local(n_leaf, n_mid, n_top, *operands):
    blocks = [x.reshape(x.shape[-2:]) for x in operands]
    r = blocks[1].shape[1]
    rows = r // n_leaf
    f32 = jnp.float32

    def pair(phases, count):
        return [pltpu.SemaphoreType.DMA((phases, count - 1))] * 2

    answer = pl.pallas_call(
        functools.partial(kernel, n_leaf, n_mid, n_top),
        out_shape=jax.ShapeDtypeStruct(blocks[-1].shape, f32),
        in_specs=[pl.BlockSpec(memory_space=pltpu.VMEM)] * len(blocks),
        out_specs=pl.BlockSpec(memory_space=pltpu.VMEM),
        scratch_shapes=[
            pltpu.VMEM((r + 2 * PANEL, r), f32),
            pltpu.VMEM((r, 9 * r), f32),
            pltpu.VMEM((n_leaf - 1, rows, 9 * r), f32),
            pltpu.VMEM((rows, 4 * r), f32),
            pltpu.VMEM((r, 4 * r), f32),
            pltpu.VMEM((rows, 5 * r), f32),
            pltpu.VMEM((n_mid - 1, rows, 5 * r), f32),
            pltpu.VMEM((rows, 5 * r), f32),
            pltpu.VMEM((r, 5 * r), f32),
            pltpu.VMEM((r, 2 * r), f32),
            pltpu.VMEM((n_top - 1, r, 2 * r), f32),
            *pair(4, n_leaf), *pair(2, n_leaf), *pair(3, n_mid), *pair(4, n_leaf), *pair(2, n_top),
        ],
        compiler_params=pltpu.CompilerParams(collective_id=0, has_side_effects=True),
    )(*blocks)
    return answer[None, None, None]


def solution(mesh):
    spread = P(("parts", "leaf"), "mid", "top", None, None)
    sizes = (mesh.shape["leaf"], mesh.shape["mid"], mesh.shape["top"])
    return jax.shard_map(
        functools.partial(local, *sizes),
        mesh=mesh,
        in_specs=(spread, spread, spread, spread, P(), P(), P(), spread),
        out_specs=spread,
        check_vma=False,
    )
```

```python
import functools

import jax
import jax.numpy as jnp
from jax import lax
from jax.experimental import pallas as pl
from jax.experimental.pallas import tpu as pltpu
from jax.sharding import PartitionSpec as P

MESH = pl.DeviceIdType.MESH
PANEL = 8


def dot(left_hand, right_side):
    return jnp.dot(
        left_hand, right_side, precision=lax.Precision.HIGHEST, preferred_element_type=jnp.float32
    )


def split3(x):
    high = x.astype(jnp.bfloat16).astype(jnp.float32)
    rest = x - high
    mid = rest.astype(jnp.bfloat16).astype(jnp.float32)
    low = (rest - mid).astype(jnp.bfloat16).astype(jnp.float32)
    return high, mid, low


def spread_panel(panel):
    p1, p2, p3 = split3(panel)
    return jnp.concatenate([p1, p1, p2, p2, p1, p3], axis=0).T.astype(jnp.bfloat16)


def rank_update(spread, scaled):
    r1, r2, r3 = split3(scaled)
    right_side = jnp.concatenate([r1, r2, r1, r2, r3, r1], axis=0).astype(jnp.bfloat16)
    return jnp.dot(spread, right_side, preferred_element_type=jnp.float32)


def negated_inverse(a_ref, matrix):
    size = matrix.shape[0]
    zero = jnp.zeros((PANEL, size), jnp.float32)
    a_ref[pl.ds(0, PANEL), :] = zero
    a_ref[pl.ds(PANEL, size), :] = matrix
    a_ref[pl.ds(PANEL + size, PANEL), :] = zero
    lane = lax.broadcasted_iota(jnp.int32, (PANEL, size), 1)
    sub = lax.broadcasted_iota(jnp.int32, (PANEL, size), 0)
    lane_full = lax.broadcasted_iota(jnp.int32, (size, size), 1)

    def columns(block, k):
        return [
            jnp.broadcast_to(
                jnp.sum(jnp.where(lane == k * PANEL + j, block, 0.0), axis=1, keepdims=True),
                block.shape,
            )
            for j in range(PANEL)
        ]

    def apply(k, spread, scaled):
        inside = (lane_full >= k * PANEL) & (lane_full < (k + 1) * PANEL)
        current = a_ref[pl.ds(PANEL, size), :]
        a_ref[pl.ds(PANEL, size), :] = jnp.where(inside, 0.0, current) - rank_update(spread, scaled)
        a_ref[pl.ds(pl.multiple_of((k + 1) * PANEL, PANEL), PANEL), :] = scaled

    def body(k, carry):
        spread_before, scaled_before, panel = carry
        apply(k - 1, spread_before, scaled_before)
        spread = spread_panel(panel)
        inside = (lane >= k * PANEL) & (lane < (k + 1) * PANEL)
        cols = columns(panel, k)
        ahead = lane == (k + 1) * PANEL + sub
        coefs = [
            jnp.broadcast_to(
                jnp.sum(
                    jnp.where(ahead, jnp.broadcast_to(panel[j : j + 1], panel.shape), 0.0),
                    axis=1, keepdims=True,
                ),
                panel.shape,
            )
            for j in range(PANEL)
        ]
        x = jnp.where(inside, jnp.where(lane - k * PANEL == sub, 1.0, 0.0), panel)
        for i in range(PANEL):
            pivot = 1.0 / jnp.broadcast_to(cols[i][i : i + 1], x.shape)
            here = sub == i

            def step(v):
                row = jnp.broadcast_to(v[i : i + 1], v.shape) * pivot
                return jnp.where(here, row, v - cols[i] * row)

            x_new = step(x)
            for j in range(i + 1, PANEL):
                cols[j] = step(cols[j])
            x = x_new
        scaled = jnp.where(inside, -x, x)
        following = a_ref[pl.ds(pl.multiple_of((k + 2) * PANEL, PANEL), PANEL), :]
        panel_next = jnp.where(inside, 0.0, following)
        for j in range(PANEL):
            panel_next = panel_next - coefs[j] * jnp.broadcast_to(scaled[j : j + 1], x.shape)
        return spread, scaled, panel_next

    steps = size // PANEL
    spread, scaled, _ = lax.fori_loop(0, steps, body, (spread_panel(zero), zero, matrix[:PANEL]))
    apply(steps - 1, spread, scaled)
    return a_ref[pl.ds(PANEL, size), :]


def kernel(
    n_leaf, n_mid, n_top,
    prec_ref, fine_ref, mid_ref, coarse_ref, core_fine_ref, core_mid_ref, core_coarse_ref, obs_ref,
    out_ref,
    a_ref, bulk_ref, rs_in, part_ref, ag_ref, piece_ref, piece_in, quarter_ref, s_ref, top_ref, top_in,
    rs_send, rs_recv, ag_send, ag_recv, mid_send, mid_recv, s_send, s_recv, top_send, top_recv,
):
    r = fine_ref.shape[1]
    rows = r // n_leaf
    leaf, mid, top = lax.axis_index("leaf"), lax.axis_index("mid"), lax.axis_index("top")
    own_rows = pl.ds(pl.multiple_of(leaf * rows, rows), rows)
    barrier = pltpu.get_barrier_semaphore()
    places = {"leaf": (leaf, n_leaf), "mid": (mid, n_mid), "top": (top, n_top)}

    far_first = sorted(range(1, n_leaf), key=lambda step: (abs(2 * step - n_leaf), step))

    def peer(axis, step):
        index, count = places[axis]
        return {axis: lax.rem(index + step, count)}

    for axis in places:
        for step in range(1, places[axis][1]):
            pl.semaphore_signal(barrier, inc=1, device_id=peer(axis, step), device_id_type=MESH)

    def send(src, dst, sems, phase, axis, step):
        copy = pltpu.make_async_remote_copy(
            src_ref=src, dst_ref=dst,
            send_sem=sems[0].at[phase, step - 1], recv_sem=sems[1].at[phase, step - 1],
            device_id=peer(axis, step), device_id_type=MESH,
        )
        copy.start()
        return copy

    def span(blocks):
        return slice(blocks[0] * r, blocks[1] * r)

    def scatter(phase, blocks):
        copies = {}
        for step in far_first:
            target = lax.rem(leaf + step, n_leaf)
            target_rows = pl.ds(pl.multiple_of(target * rows, rows), rows)
            copies[step] = send(
                bulk_ref.at[target_rows, span(blocks)], rs_in.at[step - 1, :, span(blocks)],
                (rs_send, rs_recv), phase, "leaf", step,
            )
        return copies, blocks

    def collect(handle):
        copies, blocks = handle
        total = bulk_ref[own_rows, span(blocks)]
        for step in range(1, n_leaf):
            copies[step].wait()
            total = total + rs_in[step - 1, :, span(blocks)]
        return total

    def gather(source, target, sems, phase, blocks, value):
        source[:, span(blocks)] = value
        copies = [
            send(
                source.at[:, span(blocks)], target.at[own_rows, span(blocks)],
                sems, phase, "leaf", step,
            )
            for step in far_first
        ]
        target[own_rows, span(blocks)] = value
        return copies

    def exchange(axis, source, target, sems, phase, blocks, value):
        source[:, span(blocks)] = value
        copies = [
            send(
                source.at[:, span(blocks)], target.at[step - 1, :, span(blocks)],
                sems, phase, axis, step,
            )
            for step in range(1, places[axis][1])
        ]
        return copies, target, blocks, value

    def add_up(handle):
        copies, target, blocks, total = handle
        for step, copy in enumerate(copies):
            copy.wait()
            total = total + target[step, :, span(blocks)]
        return total

    def wait_all(copies):
        for copy in copies:
            copy.wait()

    def put(place, value):
        bulk_ref[:, place * r : (place + 1) * r] = value

    prec = prec_ref[...]
    fine, middle, coarse = fine_ref[...], mid_ref[...], coarse_ref[...]
    solved_f = dot(prec, fine)
    fine_t = fine.T
    put(0, dot(fine_t, solved_f))
    pl.semaphore_wait(barrier, (n_leaf - 1) + (n_mid - 1) + (n_top - 1))
    rs_ff = scatter(0, (0, 1))
    mid_t, coarse_t = middle.T, coarse.T
    solved_y = dot(prec, obs_ref[...])
    put(1, dot(mid_t, solved_f))
    put(2, dot(coarse_t, solved_f))
    put(3, dot(fine_t, solved_y))
    rs_f = scatter(1, (1, 4))
    solved_m, solved_c = dot(prec, middle), dot(prec, coarse)
    put(4, dot(mid_t, solved_m))
    put(5, dot(mid_t, solved_c))
    put(6, dot(mid_t, solved_y))
    put(7, dot(coarse_t, solved_c))
    put(8, dot(coarse_t, solved_y))

    first = (ag_send, ag_recv)
    ag_ff = gather(part_ref, ag_ref, first, 0, (0, 1), collect(rs_ff))
    rs_m = scatter(2, (4, 7))
    part_f = collect(rs_f)
    ag_f = gather(part_ref, ag_ref, first, 1, (1, 4), part_f)
    rs_c = scatter(3, (7, 9))

    wait_all(ag_ff)
    fine_inverse = negated_inverse(a_ref, core_fine_ref[...] + ag_ref[:, :r])
    wait_all(ag_f)
    q_m, q_c = part_f[:, :r], part_f[:, r : 2 * r]
    w_m = dot(fine_inverse, ag_ref[:, r : 2 * r].T)
    part_m = collect(rs_m)
    between, second = (mid_send, mid_recv), (s_send, s_recv)
    x_mm = exchange("mid", piece_ref, piece_in, between, 0, (0, 1), part_m[:, :r] + dot(q_m, w_m))
    w_c = dot(fine_inverse, ag_ref[:, 2 * r : 3 * r].T)
    w_y = dot(fine_inverse, ag_ref[:, 3 * r : 4 * r])
    cross_piece = jnp.concatenate(
        [part_m[:, r : 2 * r] + dot(q_m, w_c), part_m[:, 2 * r :] + dot(q_m, w_y)], axis=1
    )
    x_mc = exchange("mid", piece_ref, piece_in, between, 1, (1, 3), cross_piece)
    ag_mm = gather(quarter_ref, s_ref, second, 0, (0, 1), add_up(x_mm))
    ag_mc = gather(quarter_ref, s_ref, second, 1, (1, 3), add_up(x_mc))
    part_c = collect(rs_c)
    coarse_piece = jnp.concatenate(
        [part_c[:, :r] + dot(q_c, w_c), part_c[:, r:] + dot(q_c, w_y)], axis=1
    )
    x_cc = exchange("mid", piece_ref, piece_in, between, 2, (3, 5), coarse_piece)
    coarse_sum = add_up(x_cc)
    ag_cc = gather(quarter_ref, s_ref, second, 2, (3, 4), coarse_sum[:, :r])
    ag_cy = gather(quarter_ref, s_ref, second, 3, (4, 5), coarse_sum[:, r:])

    wait_all(ag_mm)
    mid_inverse = negated_inverse(a_ref, core_mid_ref[...] + s_ref[:, :r])
    wait_all(ag_mc)
    cross = s_ref[:, r : 2 * r]
    cross_t = cross.T
    v_c = dot(mid_inverse, cross)
    last = (top_send, top_recv)
    cross_cc = dot(cross_t, v_c)
    wait_all(ag_cc)
    x_top = exchange("top", top_ref, top_in, last, 0, (0, 1), s_ref[:, 3 * r : 4 * r] + cross_cc)
    v_y = dot(mid_inverse, s_ref[:, 2 * r : 3 * r])
    cross_cy = dot(cross_t, v_y)
    wait_all(ag_cy)
    x_right = exchange("top", top_ref, top_in, last, 1, (1, 2), s_ref[:, 4 * r : 5 * r] + cross_cy)
    coarse_inverse = negated_inverse(a_ref, core_coarse_ref[...] + add_up(x_top))
    x_c = -dot(coarse_inverse, add_up(x_right))
    x_m = dot(v_c, x_c) - v_y
    x_f = dot(w_m, x_m) + dot(w_c, x_c) - w_y
    out_ref[...] = solved_y - dot(solved_f, x_f) - dot(solved_m, x_m) - dot(solved_c, x_c)


def local(n_leaf, n_mid, n_top, *operands):
    blocks = [x.reshape(x.shape[-2:]) for x in operands]
    r = blocks[1].shape[1]
    rows = r // n_leaf
    f32 = jnp.float32

    def pair(phases, count):
        return [pltpu.SemaphoreType.DMA((phases, count - 1))] * 2

    answer = pl.pallas_call(
        functools.partial(kernel, n_leaf, n_mid, n_top),
        out_shape=jax.ShapeDtypeStruct(blocks[-1].shape, f32),
        in_specs=[pl.BlockSpec(memory_space=pltpu.VMEM)] * len(blocks),
        out_specs=pl.BlockSpec(memory_space=pltpu.VMEM),
        scratch_shapes=[
            pltpu.VMEM((r + 2 * PANEL, r), f32),
            pltpu.VMEM((r, 9 * r), f32),
            pltpu.VMEM((n_leaf - 1, rows, 9 * r), f32),
            pltpu.VMEM((rows, 4 * r), f32),
            pltpu.VMEM((r, 4 * r), f32),
            pltpu.VMEM((rows, 5 * r), f32),
            pltpu.VMEM((n_mid - 1, rows, 5 * r), f32),
            pltpu.VMEM((rows, 5 * r), f32),
            pltpu.VMEM((r, 5 * r), f32),
            pltpu.VMEM((r, 2 * r), f32),
            pltpu.VMEM((n_top - 1, r, 2 * r), f32),
            *pair(4, n_leaf), *pair(2, n_leaf), *pair(3, n_mid), *pair(4, n_leaf), *pair(2, n_top),
        ],
        compiler_params=pltpu.CompilerParams(collective_id=0, has_side_effects=True),
    )(*blocks)
    return answer[None, None, None]


def solution(mesh):
    spread = P(("parts", "leaf"), "mid", "top", None, None)
    sizes = (mesh.shape["leaf"], mesh.shape["mid"], mesh.shape["top"])
    return jax.shard_map(
        functools.partial(local, *sizes),
        mesh=mesh,
        in_specs=(spread, spread, spread, spread, P(), P(), P(), spread),
        out_specs=spread,
        check_vma=False,
    )
```

```python
import functools

import jax
import jax.numpy as jnp
from jax import lax
from jax.experimental import pallas as pl
from jax.experimental.pallas import tpu as pltpu
from jax.sharding import PartitionSpec as P

MESH = pl.DeviceIdType.MESH
PANEL = 8


def dot(left_hand, right_side):
    return jnp.dot(
        left_hand, right_side, precision=lax.Precision.HIGHEST, preferred_element_type=jnp.float32
    )


def split3(x):
    high = x.astype(jnp.bfloat16).astype(jnp.float32)
    rest = x - high
    mid = rest.astype(jnp.bfloat16).astype(jnp.float32)
    low = (rest - mid).astype(jnp.bfloat16).astype(jnp.float32)
    return high, mid, low


def spread_panel(panel):
    p1, p2, p3 = split3(panel)
    return jnp.concatenate([p1, p1, p2, p2, p1, p3], axis=0).T.astype(jnp.bfloat16)


def rank_update(spread, scaled):
    r1, r2, r3 = split3(scaled)
    right_side = jnp.concatenate([r1, r2, r1, r2, r3, r1], axis=0).astype(jnp.bfloat16)
    return jnp.dot(spread, right_side, preferred_element_type=jnp.float32)


def negated_inverse(a_ref, matrix):
    size = matrix.shape[0]
    zero = jnp.zeros((PANEL, size), jnp.float32)
    a_ref[pl.ds(0, PANEL), :] = zero
    a_ref[pl.ds(PANEL, size), :] = matrix
    a_ref[pl.ds(PANEL + size, PANEL), :] = zero
    lane = lax.broadcasted_iota(jnp.int32, (PANEL, size), 1)
    sub = lax.broadcasted_iota(jnp.int32, (PANEL, size), 0)
    lane_full = lax.broadcasted_iota(jnp.int32, (size, size), 1)

    def columns(block, k):
        return [
            jnp.broadcast_to(
                jnp.sum(jnp.where(lane == k * PANEL + j, block, 0.0), axis=1, keepdims=True),
                block.shape,
            )
            for j in range(PANEL)
        ]

    def apply(k, spread, scaled):
        inside = (lane_full >= k * PANEL) & (lane_full < (k + 1) * PANEL)
        current = a_ref[pl.ds(PANEL, size), :]
        a_ref[pl.ds(PANEL, size), :] = jnp.where(inside, 0.0, current) - rank_update(spread, scaled)
        a_ref[pl.ds(pl.multiple_of((k + 1) * PANEL, PANEL), PANEL), :] = scaled

    def body(k, carry):
        spread_before, scaled_before, panel = carry
        apply(k - 1, spread_before, scaled_before)
        spread = spread_panel(panel)
        inside = (lane >= k * PANEL) & (lane < (k + 1) * PANEL)
        cols = columns(panel, k)
        ahead = lane == (k + 1) * PANEL + sub
        coefs = [
            jnp.broadcast_to(
                jnp.sum(
                    jnp.where(ahead, jnp.broadcast_to(panel[j : j + 1], panel.shape), 0.0),
                    axis=1, keepdims=True,
                ),
                panel.shape,
            )
            for j in range(PANEL)
        ]
        x = jnp.where(inside, jnp.where(lane - k * PANEL == sub, 1.0, 0.0), panel)
        for i in range(PANEL):
            pivot = 1.0 / jnp.broadcast_to(cols[i][i : i + 1], x.shape)
            here = sub == i

            def step(v):
                row = jnp.broadcast_to(v[i : i + 1], v.shape) * pivot
                return jnp.where(here, row, v - cols[i] * row)

            x_new = step(x)
            for j in range(i + 1, PANEL):
                cols[j] = step(cols[j])
            x = x_new
        scaled = jnp.where(inside, -x, x)
        following = a_ref[pl.ds(pl.multiple_of((k + 2) * PANEL, PANEL), PANEL), :]
        panel_next = jnp.where(inside, 0.0, following)
        for j in range(PANEL):
            panel_next = panel_next - coefs[j] * jnp.broadcast_to(scaled[j : j + 1], x.shape)
        return spread, scaled, panel_next

    steps = size // PANEL
    spread, scaled, _ = lax.fori_loop(0, steps, body, (spread_panel(zero), zero, matrix[:PANEL]))
    apply(steps - 1, spread, scaled)
    return a_ref[pl.ds(PANEL, size), :]


def kernel(
    n_leaf, n_mid, n_top,
    prec_ref, fine_ref, mid_ref, coarse_ref, core_fine_ref, core_mid_ref, core_coarse_ref, obs_ref,
    out_ref,
    a_ref, bulk_ref, rs_in, pair_in, cross_ref, cross_in, part_ref, ag_ref, piece_ref, piece_in, quarter_ref, s_ref, top_ref, top_in,
    rs_send, rs_recv, pair_send, pair_recv, cross_send, cross_recv, ag_send, ag_recv, mid_send, mid_recv, s_send, s_recv, top_send, top_recv,
):
    r = fine_ref.shape[1]
    rows = r // n_leaf
    leaf, mid, top = lax.axis_index("leaf"), lax.axis_index("mid"), lax.axis_index("top")
    own_rows = pl.ds(pl.multiple_of(leaf * rows, rows), rows)
    barrier = pltpu.get_barrier_semaphore()
    places = {"leaf": (leaf, n_leaf), "mid": (mid, n_mid), "top": (top, n_top)}

    far_first = sorted(range(1, n_leaf), key=lambda step: (abs(2 * step - n_leaf), step))

    def peer(axis, step):
        index, count = places[axis]
        return {axis: lax.rem(index + step, count)}

    for axis in places:
        for step in range(1, places[axis][1]):
            pl.semaphore_signal(barrier, inc=1, device_id=peer(axis, step), device_id_type=MESH)

    def send(src, dst, sems, phase, axis, step):
        copy = pltpu.make_async_remote_copy(
            src_ref=src, dst_ref=dst,
            send_sem=sems[0].at[phase, step - 1], recv_sem=sems[1].at[phase, step - 1],
            device_id=peer(axis, step), device_id_type=MESH,
        )
        copy.start()
        return copy

    def span(blocks):
        return slice(blocks[0] * r, blocks[1] * r)

    def scatter(phase, blocks):
        copies = {}
        for step in far_first:
            target = lax.rem(leaf + step, n_leaf)
            target_rows = pl.ds(pl.multiple_of(target * rows, rows), rows)
            copies[step] = send(
                bulk_ref.at[target_rows, span(blocks)], rs_in.at[step - 1, :, span(blocks)],
                (rs_send, rs_recv), phase, "leaf", step,
            )
        return copies, blocks

    def collect(handle):
        copies, blocks = handle
        total = bulk_ref[own_rows, span(blocks)]
        for step in range(1, n_leaf):
            copies[step].wait()
            total = total + rs_in[step - 1, :, span(blocks)]
        return total

    half = n_leaf // 2
    parity = lax.rem(leaf, 2)

    def row_block(index):
        return pl.ds(pl.multiple_of(index * rows, rows), rows)

    def shifted(blocks):
        return slice((blocks[0] - 4) * r, (blocks[1] - 4) * r)

    def pair_scatter(phase, blocks):
        copies = []
        for j in range(half):
            copy = pltpu.make_async_remote_copy(
                src_ref=bulk_ref.at[row_block(2 * j + 1 - parity), span(blocks)],
                dst_ref=pair_in.at[j, :, shifted(blocks)],
                send_sem=pair_send.at[phase, j], recv_sem=pair_recv.at[phase, j],
                device_id={"leaf": leaf + 1 - 2 * parity}, device_id_type=MESH,
            )
            copy.start()
            copies.append(copy)
        return copies

    def cross_scatter(phase, blocks, pair_copies):
        for copy in pair_copies:
            copy.wait()
        columns = shifted(blocks)
        copies = []
        for step in range(1, half):
            target = lax.rem(leaf + 2 * step, n_leaf)
            cross_ref[step - 1, :, columns] = (
                bulk_ref[row_block(target), span(blocks)]
                + pair_in[lax.div(target, 2), :, columns]
            )
            copy = pltpu.make_async_remote_copy(
                src_ref=cross_ref.at[step - 1, :, columns],
                dst_ref=cross_in.at[step - 1, :, columns],
                send_sem=cross_send.at[phase, step - 1], recv_sem=cross_recv.at[phase, step - 1],
                device_id={"leaf": target}, device_id_type=MESH,
            )
            copy.start()
            copies.append(copy)
        return copies, blocks

    def cross_collect(handle):
        copies, blocks = handle
        columns = shifted(blocks)
        total = bulk_ref[own_rows, span(blocks)] + pair_in[lax.div(leaf, 2), :, columns]
        for step, copy in enumerate(copies):
            copy.wait()
            total = total + cross_in[step, :, columns]
        return total

    def gather(source, target, sems, phase, blocks, value):
        source[:, span(blocks)] = value
        copies = [
            send(
                source.at[:, span(blocks)], target.at[own_rows, span(blocks)],
                sems, phase, "leaf", step,
            )
            for step in far_first
        ]
        target[own_rows, span(blocks)] = value
        return copies

    def exchange(axis, source, target, sems, phase, blocks, value):
        source[:, span(blocks)] = value
        copies = [
            send(
                source.at[:, span(blocks)], target.at[step - 1, :, span(blocks)],
                sems, phase, axis, step,
            )
            for step in range(1, places[axis][1])
        ]
        return copies, target, blocks, value

    def add_up(handle):
        copies, target, blocks, total = handle
        for step, copy in enumerate(copies):
            copy.wait()
            total = total + target[step, :, span(blocks)]
        return total

    def wait_all(copies):
        for copy in copies:
            copy.wait()

    def put(place, value):
        bulk_ref[:, place * r : (place + 1) * r] = value

    prec = prec_ref[...]
    fine, middle, coarse = fine_ref[...], mid_ref[...], coarse_ref[...]
    solved_f = dot(prec, fine)
    fine_t = fine.T
    put(0, dot(fine_t, solved_f))
    pl.semaphore_wait(barrier, (n_leaf - 1) + (n_mid - 1) + (n_top - 1))
    rs_ff = scatter(0, (0, 1))
    mid_t, coarse_t = middle.T, coarse.T
    solved_y = dot(prec, obs_ref[...])
    put(1, dot(mid_t, solved_f))
    put(2, dot(coarse_t, solved_f))
    put(3, dot(fine_t, solved_y))
    rs_f = scatter(1, (1, 4))
    solved_m, solved_c = dot(prec, middle), dot(prec, coarse)
    put(4, dot(mid_t, solved_m))
    put(5, dot(mid_t, solved_c))
    put(6, dot(mid_t, solved_y))
    put(7, dot(coarse_t, solved_c))
    put(8, dot(coarse_t, solved_y))

    first = (ag_send, ag_recv)
    ag_ff = gather(part_ref, ag_ref, first, 0, (0, 1), collect(rs_ff))
    pair_m = pair_scatter(0, (4, 7))
    part_f = collect(rs_f)
    ag_f = gather(part_ref, ag_ref, first, 1, (1, 4), part_f)
    pair_c = pair_scatter(1, (7, 9))
    rs_m = cross_scatter(0, (4, 7), pair_m)

    wait_all(ag_ff)
    fine_inverse = negated_inverse(a_ref, core_fine_ref[...] + ag_ref[:, :r])
    rs_c = cross_scatter(1, (7, 9), pair_c)
    wait_all(ag_f)
    q_m, q_c = part_f[:, :r], part_f[:, r : 2 * r]
    w_m = dot(fine_inverse, ag_ref[:, r : 2 * r].T)
    part_m = cross_collect(rs_m)
    between, second = (mid_send, mid_recv), (s_send, s_recv)
    x_mm = exchange("mid", piece_ref, piece_in, between, 0, (0, 1), part_m[:, :r] + dot(q_m, w_m))
    w_c = dot(fine_inverse, ag_ref[:, 2 * r : 3 * r].T)
    w_y = dot(fine_inverse, ag_ref[:, 3 * r : 4 * r])
    cross_piece = jnp.concatenate(
        [part_m[:, r : 2 * r] + dot(q_m, w_c), part_m[:, 2 * r :] + dot(q_m, w_y)], axis=1
    )
    x_mc = exchange("mid", piece_ref, piece_in, between, 1, (1, 3), cross_piece)
    ag_mm = gather(quarter_ref, s_ref, second, 0, (0, 1), add_up(x_mm))
    ag_mc = gather(quarter_ref, s_ref, second, 1, (1, 3), add_up(x_mc))
    part_c = cross_collect(rs_c)
    coarse_piece = jnp.concatenate(
        [part_c[:, :r] + dot(q_c, w_c), part_c[:, r:] + dot(q_c, w_y)], axis=1
    )
    x_cc = exchange("mid", piece_ref, piece_in, between, 2, (3, 5), coarse_piece)
    coarse_sum = add_up(x_cc)
    ag_cc = gather(quarter_ref, s_ref, second, 2, (3, 4), coarse_sum[:, :r])
    ag_cy = gather(quarter_ref, s_ref, second, 3, (4, 5), coarse_sum[:, r:])

    wait_all(ag_mm)
    mid_inverse = negated_inverse(a_ref, core_mid_ref[...] + s_ref[:, :r])
    wait_all(ag_mc)
    cross = s_ref[:, r : 2 * r]
    cross_t = cross.T
    v_c = dot(mid_inverse, cross)
    last = (top_send, top_recv)
    cross_cc = dot(cross_t, v_c)
    wait_all(ag_cc)
    x_top = exchange("top", top_ref, top_in, last, 0, (0, 1), s_ref[:, 3 * r : 4 * r] + cross_cc)
    v_y = dot(mid_inverse, s_ref[:, 2 * r : 3 * r])
    cross_cy = dot(cross_t, v_y)
    wait_all(ag_cy)
    x_right = exchange("top", top_ref, top_in, last, 1, (1, 2), s_ref[:, 4 * r : 5 * r] + cross_cy)
    coarse_inverse = negated_inverse(a_ref, core_coarse_ref[...] + add_up(x_top))
    x_c = -dot(coarse_inverse, add_up(x_right))
    x_m = dot(v_c, x_c) - v_y
    x_f = dot(w_m, x_m) + dot(w_c, x_c) - w_y
    out_ref[...] = solved_y - dot(solved_f, x_f) - dot(solved_m, x_m) - dot(solved_c, x_c)


def local(n_leaf, n_mid, n_top, *operands):
    blocks = [x.reshape(x.shape[-2:]) for x in operands]
    r = blocks[1].shape[1]
    rows = r // n_leaf
    half = n_leaf // 2
    f32 = jnp.float32

    def pair(phases, count):
        return [pltpu.SemaphoreType.DMA((phases, count - 1))] * 2

    answer = pl.pallas_call(
        functools.partial(kernel, n_leaf, n_mid, n_top),
        out_shape=jax.ShapeDtypeStruct(blocks[-1].shape, f32),
        in_specs=[pl.BlockSpec(memory_space=pltpu.VMEM)] * len(blocks),
        out_specs=pl.BlockSpec(memory_space=pltpu.VMEM),
        scratch_shapes=[
            pltpu.VMEM((r + 2 * PANEL, r), f32),
            pltpu.VMEM((r, 9 * r), f32),
            pltpu.VMEM((n_leaf - 1, rows, 4 * r), f32),
            pltpu.VMEM((half, rows, 5 * r), f32),
            pltpu.VMEM((half - 1, rows, 5 * r), f32),
            pltpu.VMEM((half - 1, rows, 5 * r), f32),
            pltpu.VMEM((rows, 4 * r), f32),
            pltpu.VMEM((r, 4 * r), f32),
            pltpu.VMEM((rows, 5 * r), f32),
            pltpu.VMEM((n_mid - 1, rows, 5 * r), f32),
            pltpu.VMEM((rows, 5 * r), f32),
            pltpu.VMEM((r, 5 * r), f32),
            pltpu.VMEM((r, 2 * r), f32),
            pltpu.VMEM((n_top - 1, r, 2 * r), f32),
            *pair(2, n_leaf), *pair(2, half + 1), *pair(2, half), *pair(2, n_leaf), *pair(3, n_mid), *pair(4, n_leaf), *pair(2, n_top),
        ],
        compiler_params=pltpu.CompilerParams(collective_id=0, has_side_effects=True),
    )(*blocks)
    return answer[None, None, None]


def solution(mesh):
    spread = P(("parts", "leaf"), "mid", "top", None, None)
    sizes = (mesh.shape["leaf"], mesh.shape["mid"], mesh.shape["top"])
    return jax.shard_map(
        functools.partial(local, *sizes),
        mesh=mesh,
        in_specs=(spread, spread, spread, spread, P(), P(), P(), spread),
        out_specs=spread,
        check_vma=False,
    )
```

```python
import functools

import jax
import jax.numpy as jnp
from jax import lax
from jax.experimental import pallas as pl
from jax.experimental.pallas import tpu as pltpu
from jax.sharding import PartitionSpec as P

MESH = pl.DeviceIdType.MESH
PANEL = 8


def dot(left_hand, right_side):
    return jnp.dot(
        left_hand, right_side, precision=lax.Precision.HIGHEST, preferred_element_type=jnp.float32
    )


def split3(x):
    high = x.astype(jnp.bfloat16).astype(jnp.float32)
    rest = x - high
    mid = rest.astype(jnp.bfloat16).astype(jnp.float32)
    low = (rest - mid).astype(jnp.bfloat16).astype(jnp.float32)
    return high, mid, low


def spread_panel(panel):
    p1, p2, p3 = split3(panel)
    return jnp.concatenate([p1, p1, p2, p2, p1, p3], axis=0).T.astype(jnp.bfloat16)


def rank_update(spread, scaled):
    r1, r2, r3 = split3(scaled)
    right_side = jnp.concatenate([r1, r2, r1, r2, r3, r1], axis=0).astype(jnp.bfloat16)
    return jnp.dot(spread, right_side, preferred_element_type=jnp.float32)


def negated_inverse(a_ref, matrix):
    size = matrix.shape[0]
    zero = jnp.zeros((PANEL, size), jnp.float32)
    a_ref[pl.ds(0, PANEL), :] = zero
    a_ref[pl.ds(PANEL, size), :] = matrix
    a_ref[pl.ds(PANEL + size, PANEL), :] = zero
    lane = lax.broadcasted_iota(jnp.int32, (PANEL, size), 1)
    sub = lax.broadcasted_iota(jnp.int32, (PANEL, size), 0)
    lane_full = lax.broadcasted_iota(jnp.int32, (size, size), 1)

    def columns(block, k):
        return [
            jnp.broadcast_to(
                jnp.sum(jnp.where(lane == k * PANEL + j, block, 0.0), axis=1, keepdims=True),
                block.shape,
            )
            for j in range(PANEL)
        ]

    def apply(k, spread, scaled):
        inside = (lane_full >= k * PANEL) & (lane_full < (k + 1) * PANEL)
        current = a_ref[pl.ds(PANEL, size), :]
        a_ref[pl.ds(PANEL, size), :] = jnp.where(inside, 0.0, current) - rank_update(spread, scaled)
        a_ref[pl.ds(pl.multiple_of((k + 1) * PANEL, PANEL), PANEL), :] = scaled

    def body(k, carry):
        spread_before, scaled_before, panel = carry
        apply(k - 1, spread_before, scaled_before)
        spread = spread_panel(panel)
        inside = (lane >= k * PANEL) & (lane < (k + 1) * PANEL)
        cols = columns(panel, k)
        ahead = lane == (k + 1) * PANEL + sub
        coefs = [
            jnp.broadcast_to(
                jnp.sum(
                    jnp.where(ahead, jnp.broadcast_to(panel[j : j + 1], panel.shape), 0.0),
                    axis=1, keepdims=True,
                ),
                panel.shape,
            )
            for j in range(PANEL)
        ]
        x = jnp.where(inside, jnp.where(lane - k * PANEL == sub, 1.0, 0.0), panel)
        for i in range(PANEL):
            pivot = 1.0 / jnp.broadcast_to(cols[i][i : i + 1], x.shape)
            here = sub == i

            def step(v):
                row = jnp.broadcast_to(v[i : i + 1], v.shape) * pivot
                return jnp.where(here, row, v - cols[i] * row)

            x_new = step(x)
            for j in range(i + 1, PANEL):
                cols[j] = step(cols[j])
            x = x_new
        scaled = jnp.where(inside, -x, x)
        following = a_ref[pl.ds(pl.multiple_of((k + 2) * PANEL, PANEL), PANEL), :]
        panel_next = jnp.where(inside, 0.0, following)
        for j in range(PANEL):
            panel_next = panel_next - coefs[j] * jnp.broadcast_to(scaled[j : j + 1], x.shape)
        return spread, scaled, panel_next

    steps = size // PANEL
    spread, scaled, _ = lax.fori_loop(0, steps, body, (spread_panel(zero), zero, matrix[:PANEL]))
    apply(steps - 1, spread, scaled)
    return a_ref[pl.ds(PANEL, size), :]


def kernel(
    n_leaf, n_mid, n_top,
    prec_ref, fine_ref, mid_ref, coarse_ref, core_fine_ref, core_mid_ref, core_coarse_ref, obs_ref,
    out_ref,
    a_ref, bulk_ref, rs_in, pair_in, cross_ref, cross_in, part_ref, ag_ref, piece_ref, piece_in, quarter_ref, s_ref, top_ref, top_in,
    rs_send, rs_recv, pair_send, pair_recv, cross_send, cross_recv, ag_send, ag_recv, mid_send, mid_recv, s_send, s_recv, top_send, top_recv,
):
    r = fine_ref.shape[1]
    rows = r // n_leaf
    leaf, mid, top = lax.axis_index("leaf"), lax.axis_index("mid"), lax.axis_index("top")
    own_rows = pl.ds(pl.multiple_of(leaf * rows, rows), rows)
    barrier = pltpu.get_barrier_semaphore()
    places = {"leaf": (leaf, n_leaf), "mid": (mid, n_mid), "top": (top, n_top)}

    far_first = sorted(range(1, n_leaf), key=lambda step: (abs(2 * step - n_leaf), step))

    def peer(axis, step):
        index, count = places[axis]
        return {axis: lax.rem(index + step, count)}

    for axis in places:
        for step in range(1, places[axis][1]):
            pl.semaphore_signal(barrier, inc=1, device_id=peer(axis, step), device_id_type=MESH)

    def send(src, dst, sems, phase, axis, step):
        copy = pltpu.make_async_remote_copy(
            src_ref=src, dst_ref=dst,
            send_sem=sems[0].at[phase, step - 1], recv_sem=sems[1].at[phase, step - 1],
            device_id=peer(axis, step), device_id_type=MESH,
        )
        copy.start()
        return copy

    def span(blocks):
        return slice(blocks[0] * r, blocks[1] * r)

    def scatter(phase, blocks):
        copies = {}
        for step in far_first:
            target = lax.rem(leaf + step, n_leaf)
            target_rows = pl.ds(pl.multiple_of(target * rows, rows), rows)
            copies[step] = send(
                bulk_ref.at[target_rows, span(blocks)], rs_in.at[step - 1, :, span(blocks)],
                (rs_send, rs_recv), phase, "leaf", step,
            )
        return copies, blocks

    def collect(handle):
        copies, blocks = handle
        total = bulk_ref[own_rows, span(blocks)]
        for step in range(1, n_leaf):
            copies[step].wait()
            total = total + rs_in[step - 1, :, span(blocks)]
        return total

    half = n_leaf // 2
    parity = lax.rem(leaf, 2)

    def row_block(index):
        return pl.ds(pl.multiple_of(index * rows, rows), rows)

    def shifted(blocks):
        return slice((blocks[0] - 4) * r, (blocks[1] - 4) * r)

    def pair_scatter(phase, blocks):
        copies = []
        for j in range(half):
            copy = pltpu.make_async_remote_copy(
                src_ref=bulk_ref.at[row_block(2 * j + 1 - parity), span(blocks)],
                dst_ref=pair_in.at[j, :, shifted(blocks)],
                send_sem=pair_send.at[phase, j], recv_sem=pair_recv.at[phase, j],
                device_id={"leaf": leaf + 1 - 2 * parity}, device_id_type=MESH,
            )
            copy.start()
            copies.append(copy)
        return copies

    def cross_scatter(phase, blocks, pair_copies):
        for copy in pair_copies:
            copy.wait()
        columns = shifted(blocks)
        copies = []
        for step in range(1, half):
            target = lax.rem(leaf + 2 * step, n_leaf)
            cross_ref[step - 1, :, columns] = (
                bulk_ref[row_block(target), span(blocks)]
                + pair_in[lax.div(target, 2), :, columns]
            )
            copy = pltpu.make_async_remote_copy(
                src_ref=cross_ref.at[step - 1, :, columns],
                dst_ref=cross_in.at[step - 1, :, columns],
                send_sem=cross_send.at[phase, step - 1], recv_sem=cross_recv.at[phase, step - 1],
                device_id={"leaf": target}, device_id_type=MESH,
            )
            copy.start()
            copies.append(copy)
        return copies, blocks

    def cross_collect(handle):
        copies, blocks = handle
        columns = shifted(blocks)
        total = bulk_ref[own_rows, span(blocks)] + pair_in[lax.div(leaf, 2), :, columns]
        for step, copy in enumerate(copies):
            copy.wait()
            total = total + cross_in[step, :, columns]
        return total

    def gather(source, target, sems, phase, blocks, value):
        source[:, span(blocks)] = value
        copies = [
            send(
                source.at[:, span(blocks)], target.at[own_rows, span(blocks)],
                sems, phase, "leaf", step,
            )
            for step in far_first
        ]
        target[own_rows, span(blocks)] = value
        return copies

    def exchange(axis, source, target, sems, phase, blocks, value):
        source[:, span(blocks)] = value
        copies = [
            send(
                source.at[:, span(blocks)], target.at[step - 1, :, span(blocks)],
                sems, phase, axis, step,
            )
            for step in range(1, places[axis][1])
        ]
        return copies, target, blocks, value

    def add_up(handle):
        copies, target, blocks, total = handle
        for step, copy in enumerate(copies):
            copy.wait()
            total = total + target[step, :, span(blocks)]
        return total

    def wait_all(copies):
        for copy in copies:
            copy.wait()

    def put(place, value):
        bulk_ref[:, place * r : (place + 1) * r] = value

    prec = prec_ref[...]
    fine, middle, coarse = fine_ref[...], mid_ref[...], coarse_ref[...]
    solved_f = dot(prec, fine)
    fine_t = fine.T
    put(0, dot(fine_t, solved_f))
    pl.semaphore_wait(barrier, (n_leaf - 1) + (n_mid - 1) + (n_top - 1))
    rs_ff = scatter(0, (0, 1))
    mid_t, coarse_t = middle.T, coarse.T
    solved_y = dot(prec, obs_ref[...])
    put(1, dot(mid_t, solved_f))
    put(2, dot(coarse_t, solved_f))
    put(3, dot(fine_t, solved_y))
    rs_f = scatter(1, (1, 4))
    solved_m, solved_c = dot(prec, middle), dot(prec, coarse)
    put(4, dot(mid_t, solved_m))
    put(5, dot(mid_t, solved_c))
    put(6, dot(mid_t, solved_y))
    put(7, dot(coarse_t, solved_c))
    put(8, dot(coarse_t, solved_y))

    first = (ag_send, ag_recv)
    ag_ff = gather(part_ref, ag_ref, first, 0, (0, 1), collect(rs_ff))
    pair_m = pair_scatter(0, (4, 7))
    part_f = collect(rs_f)
    ag_mf = gather(part_ref, ag_ref, first, 1, (1, 2), part_f[:, :r])
    ag_f = gather(part_ref, ag_ref, first, 2, (2, 4), part_f[:, r:])
    pair_c = pair_scatter(1, (7, 9))
    rs_m = cross_scatter(0, (4, 7), pair_m)

    wait_all(ag_ff)
    fine_inverse = negated_inverse(a_ref, core_fine_ref[...] + ag_ref[:, :r])
    rs_c = cross_scatter(1, (7, 9), pair_c)
    wait_all(ag_mf)
    q_m, q_c = part_f[:, :r], part_f[:, r : 2 * r]
    w_m = dot(fine_inverse, ag_ref[:, r : 2 * r].T)
    part_m = cross_collect(rs_m)
    between, second = (mid_send, mid_recv), (s_send, s_recv)
    x_mm = exchange("mid", piece_ref, piece_in, between, 0, (0, 1), part_m[:, :r] + dot(q_m, w_m))
    ag_mm = gather(quarter_ref, s_ref, second, 0, (0, 1), add_up(x_mm))
    wait_all(ag_f)
    w_c = dot(fine_inverse, ag_ref[:, 2 * r : 3 * r].T)
    w_y = dot(fine_inverse, ag_ref[:, 3 * r : 4 * r])
    cross_piece = jnp.concatenate(
        [part_m[:, r : 2 * r] + dot(q_m, w_c), part_m[:, 2 * r :] + dot(q_m, w_y)], axis=1
    )
    x_mc = exchange("mid", piece_ref, piece_in, between, 1, (1, 3), cross_piece)
    ag_mc = gather(quarter_ref, s_ref, second, 1, (1, 3), add_up(x_mc))
    part_c = cross_collect(rs_c)
    coarse_piece = jnp.concatenate(
        [part_c[:, :r] + dot(q_c, w_c), part_c[:, r:] + dot(q_c, w_y)], axis=1
    )
    x_cc = exchange("mid", piece_ref, piece_in, between, 2, (3, 5), coarse_piece)
    coarse_sum = add_up(x_cc)
    ag_cc = gather(quarter_ref, s_ref, second, 2, (3, 4), coarse_sum[:, :r])
    ag_cy = gather(quarter_ref, s_ref, second, 3, (4, 5), coarse_sum[:, r:])

    wait_all(ag_mm)
    mid_inverse = negated_inverse(a_ref, core_mid_ref[...] + s_ref[:, :r])
    wait_all(ag_mc)
    cross = s_ref[:, r : 2 * r]
    cross_t = cross.T
    v_c = dot(mid_inverse, cross)
    last = (top_send, top_recv)
    cross_cc = dot(cross_t, v_c)
    wait_all(ag_cc)
    x_top = exchange("top", top_ref, top_in, last, 0, (0, 1), s_ref[:, 3 * r : 4 * r] + cross_cc)
    v_y = dot(mid_inverse, s_ref[:, 2 * r : 3 * r])
    cross_cy = dot(cross_t, v_y)
    wait_all(ag_cy)
    x_right = exchange("top", top_ref, top_in, last, 1, (1, 2), s_ref[:, 4 * r : 5 * r] + cross_cy)
    coarse_inverse = negated_inverse(a_ref, core_coarse_ref[...] + add_up(x_top))
    x_c = -dot(coarse_inverse, add_up(x_right))
    x_m = dot(v_c, x_c) - v_y
    x_f = dot(w_m, x_m) + dot(w_c, x_c) - w_y
    out_ref[...] = solved_y - dot(solved_f, x_f) - dot(solved_m, x_m) - dot(solved_c, x_c)


def local(n_leaf, n_mid, n_top, *operands):
    blocks = [x.reshape(x.shape[-2:]) for x in operands]
    r = blocks[1].shape[1]
    rows = r // n_leaf
    half = n_leaf // 2
    f32 = jnp.float32

    def pair(phases, count):
        return [pltpu.SemaphoreType.DMA((phases, count - 1))] * 2

    answer = pl.pallas_call(
        functools.partial(kernel, n_leaf, n_mid, n_top),
        out_shape=jax.ShapeDtypeStruct(blocks[-1].shape, f32),
        in_specs=[pl.BlockSpec(memory_space=pltpu.VMEM)] * len(blocks),
        out_specs=pl.BlockSpec(memory_space=pltpu.VMEM),
        scratch_shapes=[
            pltpu.VMEM((r + 2 * PANEL, r), f32),
            pltpu.VMEM((r, 9 * r), f32),
            pltpu.VMEM((n_leaf - 1, rows, 4 * r), f32),
            pltpu.VMEM((half, rows, 5 * r), f32),
            pltpu.VMEM((half - 1, rows, 5 * r), f32),
            pltpu.VMEM((half - 1, rows, 5 * r), f32),
            pltpu.VMEM((rows, 4 * r), f32),
            pltpu.VMEM((r, 4 * r), f32),
            pltpu.VMEM((rows, 5 * r), f32),
            pltpu.VMEM((n_mid - 1, rows, 5 * r), f32),
            pltpu.VMEM((rows, 5 * r), f32),
            pltpu.VMEM((r, 5 * r), f32),
            pltpu.VMEM((r, 2 * r), f32),
            pltpu.VMEM((n_top - 1, r, 2 * r), f32),
            *pair(2, n_leaf), *pair(2, half + 1), *pair(2, half), *pair(3, n_leaf), *pair(3, n_mid), *pair(4, n_leaf), *pair(2, n_top),
        ],
        compiler_params=pltpu.CompilerParams(collective_id=0, has_side_effects=True),
    )(*blocks)
    return answer[None, None, None]


def solution(mesh):
    spread = P(("parts", "leaf"), "mid", "top", None, None)
    sizes = (mesh.shape["leaf"], mesh.shape["mid"], mesh.shape["top"])
    return jax.shard_map(
        functools.partial(local, *sizes),
        mesh=mesh,
        in_specs=(spread, spread, spread, spread, P(), P(), P(), spread),
        out_specs=spread,
        check_vma=False,
    )
```
